32 devices in a mesh: gx: 4 (over y, x), gy: 8 (over z, core).
Axes of the slice: x: 2, y: 2, z: 4, core: 2. Of those that a mesh axis runs over, the one named last changes fastest.
Arguments:
- source_values: bfloat16 [4096, 64, 128], P(('gx', 'gy')), may hold values from -6 to 6
- leaf_maps: bfloat16 [4096, 32, 128], P(('gx', 'gy')), may hold values from -0.5 to 0.5
- source_transfers: bfloat16 [4, 4096, 32, 128], P(None, ('gx', 'gy')), may hold values from -0.5 to 0.5
- target_transfers: bfloat16 [4, 4096, 32, 128], P(None, ('gx', 'gy')), may hold values from -0.5 to 0.5
Outputs:
- target_coeffs: bfloat16 [4096, 32, 128], P(('gx', 'gy'))
The draws below stay inside these ranges and needn't reach their ends.
All inputs are finite; a program needn't handle non-finite values.
Results may differ from the reference program's by a relative error of at most 0.012.
Values may be sent and summed in bfloat16 or wider, within the bound.
No kernel may reach another device: no remote copies, remote signals or barrier semaphores. Data moves between devices by JAX's collectives and lax.ppermute only.
A program may use at most 128 MiB of HBM per device.

```python
import jax
import jax.numpy as jnp
from jax import lax

RANK = 32
RHS = 64
LEAF = 64
BOX_DEV = 128
LEV = 4
COLS = 128
BOXES = 4096
N_GX = 4
N_GY = 8


def block_scale(rng, shape, shards, smallest, top_value):
    def one(position, parts):
        steps = jax.random.uniform(jax.random.fold_in(jax.random.fold_in(rng, 6), position), (parts,), jnp.float32, smallest / len(shards), top_value / len(shards))
        return jnp.repeat(jnp.exp(steps), shape[position] // parts).reshape((-1,) + (1,) * (len(shape) - position - 1))

    factor_of = one(*shards[0])
    for cut in shards[1:]:
        factor_of = factor_of * one(*cut)
    return factor_of


def bell_draw(own_key, extent, scale, limit, cuts=(), held_as=jnp.bfloat16):
    drawn = jax.random.normal(own_key, extent, jnp.float32) * scale
    if len(cuts) > 0:
        drawn = block_scale(own_key, extent, cuts, -0.22, 0.18) * drawn
    return jnp.clip(drawn, min=-limit, max=limit).astype(held_as)


def setup_inputs(seed: int = 0) -> dict:
    key_list = jax.random.split(jax.random.key(seed), 5)
    source_values = bell_draw(key_list[0], (BOXES, LEAF, COLS), 1.0, 6.0, ((0, 32),))
    leaf_maps = bell_draw(key_list[1], (BOXES, RANK, 2 * LEAF), (2 * LEAF) ** -0.5, 0.5, ((0, 32),))
    source_transfers = bell_draw(key_list[2], (LEV, BOXES, RANK, 4 * RANK), (4 * RANK) ** -0.5, 0.5, ((1, 32),))
    target_transfers = bell_draw(key_list[3], (LEV, BOXES, RANK, 4 * RANK), (4 * RANK) ** -0.5, 0.5, ((1, 32),))
    return {"source_values": source_values, "leaf_maps": leaf_maps, "source_transfers": source_transfers, "target_transfers": target_transfers}


def combine(product):
    nboxes, _, rank_n, cols = product.shape
    pieces = product.reshape(nboxes, 2, rank_n, cols // (2 * RHS), 2, RHS)
    real_part = pieces[:, 0, :, :, 0] - pieces[:, 1, :, :, 1]
    imag_part = pieces[:, 0, :, :, 1] + pieces[:, 1, :, :, 0]
    return jnp.stack([real_part, imag_part], axis=3).reshape(nboxes, rank_n, cols).astype(jnp.bfloat16)


def leaf_step(operands):
    maps_block, values_block = operands
    nboxes, rank_n, width = maps_block.shape
    split = maps_block.reshape(nboxes, rank_n, 2, width // 2).astype(jnp.float32)
    product = jnp.einsum('bipj,bjc->bpic', split, values_block.astype(jnp.float32))
    return combine(product)


def transfer_step(operands):
    coeffs, partner, transfer = operands
    nboxes, rank_n, cols = coeffs.shape
    stacked = jnp.stack([coeffs, partner], axis=1).astype(jnp.float32)
    blocks = transfer.reshape(nboxes, rank_n, 2, 2, rank_n).astype(jnp.float32)
    return combine(jnp.einsum('bispj,bsjc->bpic', blocks, stacked))


def partner_of(coeffs, device_bit):
    span = BOX_DEV * (2 ** device_bit)
    grouped = coeffs.reshape((coeffs.shape[0] // (2 * span), 2, span) + coeffs.shape[1:])
    return grouped[:, ::-1].reshape(coeffs.shape)


def blocked(array):
    devices_n = N_GX * N_GY
    return array.reshape((devices_n, BOX_DEV) + array.shape[1:])


def apply_level(coeffs, transfer, device_bit):
    partner = partner_of(coeffs, device_bit)
    result = lax.map(transfer_step, (blocked(coeffs), blocked(partner), blocked(transfer)))
    return result.reshape(coeffs.shape)


def reference(source_values, leaf_maps, source_transfers, target_transfers):
    devices_n = N_GX * N_GY
    all_bits = devices_n.bit_length() - 1
    coeffs = lax.map(leaf_step, (blocked(leaf_maps), blocked(source_values)))
    coeffs = coeffs.reshape(BOXES, RANK, COLS)
    for level_no in range(LEV):
        coeffs = apply_level(coeffs, source_transfers[level_no], level_no % all_bits)
    piece = BOX_DEV // devices_n
    coeffs = coeffs.reshape(devices_n, devices_n, piece, RANK, COLS).transpose(1, 0, 2, 3, 4).reshape(BOXES, RANK, COLS)
    for level_no in range(LEV):
        coeffs = apply_level(coeffs, target_transfers[level_no], (all_bits - 1 - level_no) % all_bits)
    return coeffs
```

```python
import functools

import jax
import jax.numpy as jnp
from jax import lax
from jax.experimental import pallas as pl
from jax.experimental.pallas import tpu as pltpu
from jax.sharding import PartitionSpec as P

CHUNKS = 4
STEP_BOXES = 16


def swapped(block, axis, apart):
    count = lax.axis_size(axis)
    route = []
    for low in range(count):
        high = low | 1 << apart
        if high != low and high < count:
            route += [(low, high), (high, low)]
    return lax.ppermute(block, axis, route)


def turned(block):
    wide = block.astype(jnp.float32)
    cols = wide.shape[-1]
    lane = lax.broadcasted_iota(jnp.int32, wide.shape, 1)
    rolled = pltpu.roll(wide, cols // 2, 1)
    return jnp.where(lane < cols // 2, -rolled, rolled).astype(block.dtype)


def apply_kernel(*refs):
    operand_refs, matrix_ref, out_ref = refs[:-2], refs[-2], refs[-1]
    count, width = out_ref.shape[0], out_ref.shape[1]
    for v in range(count):
        for w in range(width):
            rows = []
            for ref in operand_refs:
                block = ref[v, w]
                rows += [block, turned(block)]
            operand = jnp.concatenate(rows, axis=0)
            out_ref[v, w] = jnp.dot(
                matrix_ref[v, w], operand, preferred_element_type=jnp.float32
            ).astype(out_ref.dtype)


def complex_apply(operands, matrix, level, chunk, width, operand_chunk):
    count = operands[0].shape[0]
    rank, inner = matrix.shape[-2:]
    cols = operands[0].shape[-1]
    step = max(1, min(count, STEP_BOXES // width))
    in_specs = []
    for operand in operands:
        in_specs.append(
            pl.BlockSpec((step, width) + operand.shape[2:], lambda s: (s, operand_chunk, 0, 0))
        )
    if level is None:
        in_specs.append(pl.BlockSpec((step, width, rank, inner), lambda s: (s, chunk, 0, 0)))
    else:
        in_specs.append(
            pl.BlockSpec((None, step, width, rank, inner), lambda s: (level, s, chunk, 0, 0))
        )
    flops = 2 * count * width * rank * inner * cols
    return pl.pallas_call(
        apply_kernel,
        grid=(count // step,),
        in_specs=in_specs,
        out_specs=pl.BlockSpec((step, width, rank, cols), lambda s: (s, 0, 0, 0)),
        out_shape=jax.ShapeDtypeStruct((count, width, rank, cols), operands[0].dtype),
        cost_estimate=pl.CostEstimate(
            flops=flops, bytes_accessed=4 * 2 * count * width * rank * cols, transcendentals=0
        ),
    )(*operands, matrix)


def local(source_values, leaf_maps, source_transfers, target_transfers):
    devices_n = lax.axis_size("gx") * lax.axis_size("gy")
    low_bits = lax.axis_size("gy").bit_length() - 1
    all_bits = low_bits + lax.axis_size("gx").bit_length() - 1
    levels, boxes = source_transfers.shape[:2]
    piece = boxes // devices_n
    chunks = min(CHUNKS, piece)
    width = piece // chunks

    def split(array, at):
        shape = array.shape
        return array.reshape(shape[:at] + (devices_n, piece) + shape[at + 1 :])

    source_values = split(source_values, 0)
    leaf_maps = split(leaf_maps, 0)
    source_transfers = split(source_transfers, 1)
    target_transfers = split(target_transfers, 1)

    def partner_of(coeffs, device_bit):
        if device_bit < low_bits:
            return swapped(coeffs, "gy", device_bit)
        return swapped(coeffs, "gx", device_bit - low_bits)

    state = [
        complex_apply([source_values], leaf_maps, None, c, width, c) for c in range(chunks)
    ]
    for side, transfers in enumerate((source_transfers, target_transfers)):
        for level_no in range(levels):
            bit = level_no % all_bits if side == 0 else (all_bits - 1 - level_no) % all_bits
            for c in range(chunks):
                partner = partner_of(state[c], bit)
                state[c] = complex_apply([state[c], partner], transfers, level_no, c, width, 0)
        if side == 0:
            state = [
                lax.all_to_all(block, ("gx", "gy"), split_axis=0, concat_axis=0, tiled=True)
                for block in state
            ]
    coeffs = jnp.concatenate(state, axis=1)
    return coeffs.reshape((boxes,) + coeffs.shape[2:])


def solution(mesh):
    return jax.shard_map(
        local,
        mesh=mesh,
        in_specs=(
            P(("gx", "gy"), None, None),
            P(("gx", "gy"), None, None),
            P(None, ("gx", "gy"), None, None),
            P(None, ("gx", "gy"), None, None),
        ),
        out_specs=P(("gx", "gy"), None, None),
        check_vma=False,
    )
```

```python
import functools

import jax
import jax.numpy as jnp
from jax import lax
from jax.experimental import pallas as pl
from jax.experimental.pallas import tpu as pltpu
from jax.sharding import PartitionSpec as P


CHUNKS = 4
LAG = 1
VMEM_BYTES = 8 * 1024 * 1024
STEP_BOXES = 16


def swapped(block, axis, apart):
    count = lax.axis_size(axis)
    route = []
    for low in range(count):
        high = low | 1 << apart
        if high != low and high < count:
            route += [(low, high), (high, low)]
    return lax.ppermute(block, axis, route)


def turned(block):
    wide = block.astype(jnp.float32)
    cols = wide.shape[-1]
    lane = lax.broadcasted_iota(jnp.int32, wide.shape, 1)
    rolled = pltpu.roll(wide, cols // 2, 1)
    return jnp.where(lane < cols // 2, -rolled, rolled).astype(block.dtype)


def apply_kernel(*refs):
    operand_refs, matrix_ref, out_ref = refs[:-2], refs[-2], refs[-1]
    count, width = out_ref.shape[0], out_ref.shape[1]
    for v in range(count):
        for w in range(width):
            rows = []
            for ref in operand_refs:
                block = ref[v, w]
                rows += [block, turned(block)]
            operand = jnp.concatenate(rows, axis=0)
            out_ref[v, w] = jnp.dot(
                matrix_ref[v, w], operand, preferred_element_type=jnp.float32
            ).astype(out_ref.dtype)


def complex_apply(operands, matrix, level, chunk, width, operand_chunk):
    count = operands[0].shape[0]
    rank, inner = matrix.shape[-2:]
    cols = operands[0].shape[-1]
    step = max(1, min(count, STEP_BOXES // width))
    in_specs = []
    for operand in operands:
        in_specs.append(
            pl.BlockSpec((step, width) + operand.shape[2:], lambda s: (s, operand_chunk, 0, 0))
        )
    if level is None:
        in_specs.append(pl.BlockSpec((step, width, rank, inner), lambda s: (s, chunk, 0, 0)))
    else:
        in_specs.append(
            pl.BlockSpec((None, step, width, rank, inner), lambda s: (level, s, chunk, 0, 0))
        )
    flops = 2 * count * width * rank * inner * cols
    return pl.pallas_call(
        apply_kernel,
        grid=(count // step,),
        in_specs=in_specs,
        out_specs=pl.BlockSpec((step, width, rank, cols), lambda s: (s, 0, 0, 0)),
        compiler_params=pltpu.CompilerParams(vmem_limit_bytes=VMEM_BYTES),
        out_shape=jax.ShapeDtypeStruct((count, width, rank, cols), operands[0].dtype),
        cost_estimate=pl.CostEstimate(
            flops=flops, bytes_accessed=4 * 2 * count * width * rank * cols, transcendentals=0
        ),
    )(*operands, matrix)


def stage_list(levels, all_bits):
    source = [(0, n, n % all_bits) for n in range(levels)]
    target = [(1, n, (all_bits - 1 - n) % all_bits) for n in range(levels)]
    return source + [(None, None, None)] + target


def issue_order(chunks, stages):
    order = []
    for step in range(stages + LAG * (chunks - 1)):
        for c in reversed(range(chunks)):
            if 0 <= step - LAG * c < stages:
                order.append((c, step - LAG * c))
    return order


def chunk_count(boxes, devices_n):
    return min(CHUNKS, boxes // devices_n)


def local(source_values, leaf_maps, source_transfers, target_transfers):
    devices_n = lax.axis_size("gx") * lax.axis_size("gy")
    low_bits = lax.axis_size("gy").bit_length() - 1
    all_bits = low_bits + lax.axis_size("gx").bit_length() - 1
    levels, boxes = source_transfers.shape[:2]
    piece = boxes // devices_n
    chunks = chunk_count(boxes, devices_n)
    width = piece // chunks

    def split(array, at):
        shape = array.shape
        return array.reshape(shape[:at] + (devices_n, piece) + shape[at + 1 :])

    source_values = split(source_values, 0)
    leaf_maps = split(leaf_maps, 0)
    source_transfers = split(source_transfers, 1)
    target_transfers = split(target_transfers, 1)

    def partner_of(coeffs, device_bit):
        if device_bit < low_bits:
            return swapped(coeffs, "gy", device_bit)
        return swapped(coeffs, "gx", device_bit - low_bits)

    stages = stage_list(levels, all_bits)
    state = [
        complex_apply([source_values], leaf_maps, None, c, width, c) for c in range(chunks)
    ]
    for c, s in issue_order(chunks, len(stages)):
        side, level_no, bit = stages[s]
        if side is None:
            state[c] = lax.all_to_all(
                state[c], ("gx", "gy"), split_axis=0, concat_axis=0, tiled=True
            )
            continue
        partner = partner_of(state[c], bit)
        transfers = (source_transfers, target_transfers)[side]
        state[c] = complex_apply([state[c], partner], transfers, level_no, c, width, 0)
    coeffs = jnp.concatenate(state, axis=1)
    return coeffs.reshape((boxes,) + coeffs.shape[2:])


def whole(mesh, source_values, leaf_maps, source_transfers, target_transfers):
    step = jax.shard_map(
        local,
        mesh=mesh,
        in_specs=(
            P(("gx", "gy"), None, None),
            P(("gx", "gy"), None, None),
            P(None, ("gx", "gy"), None, None),
            P(None, ("gx", "gy"), None, None),
        ),
        out_specs=P(("gx", "gy"), None, None),
        check_vma=False,
    )
    return step(source_values, leaf_maps, source_transfers, target_transfers)


def solution(mesh):
    return functools.partial(whole, mesh)
```
